32 devices in a mesh: level: 8 (over z, core), member: 4 (over y, x).
Axes of the slice: x: 2, y: 2, z: 4, core: 2. Of those that a mesh axis runs over, the one named last changes fastest.
Arguments:
- model_state: float32 [4, 32, 4, 256, 512], P('member', 'level'), may hold values from -6 to 6
- noise_field: bfloat16 [4, 32, 4, 256, 512], P('member', 'level'), may hold values from -5 to 5
- cotangent: bfloat16 [4, 32, 4, 256, 512], P('member', 'level'), may hold values from -6 to 6
- zonal_shift: float32 [32, 4], P('level'), may hold values from -0.02 to 0.02
- viscosity: float32 [32, 4], P('level'), may hold values from 0.1 to 3
- noise_scale: float32 [32, 4], P('level'), may hold values from 0.2 to 1
- w_in: bfloat16 [128, 384], replicated, may hold values from -0.5 to 0.5
- b_in: float32 [384], replicated, may hold values from -3 to 3
- w_mid: bfloat16 [384, 384], replicated, may hold values from -0.3125 to 0.3125
- b_mid: float32 [384], replicated, may hold values from -3 to 3
- w_out: bfloat16 [384, 128], replicated, may hold values from -0.3125 to 0.3125
Outputs:
- next_state: float32 [4, 32, 4, 256, 512], P('member', 'level')
- state_grad: float32 [4, 32, 4, 256, 512], P('member', 'level')
- grad_w_in: float32 [128, 384], P(None, ('level', 'member'))
- grad_w_mid: float32 [384, 384], P(None, ('level', 'member'))
- grad_w_out: float32 [128, 384], P(None, ('level', 'member'))
- grad_bias: float32 [2, 384], P(None, ('level', 'member'))
The draws below stay inside these ranges and needn't reach their ends.
All inputs are finite; a program needn't handle non-finite values.
Results may differ from the reference program's by a relative error of at most 0.0085.
Values may be sent and summed in bfloat16 or wider, within the bound.
No kernel may reach another device: no remote copies, remote signals or barrier semaphores. Data moves between devices by JAX's collectives and lax.ppermute only.
A program may use at most 192 MiB of HBM per device.

```python
import math
import jax
import jax.numpy as jnp
from jax import lax

L = 32
F = 4
NLAT = 256
NLON = 512
WAVES = 128
MODES = 128
H = 384
MEMBERS = 4
HIN = 128
HOUT = 128


def levels(own_key, extent, shards, low, top_value):
    def one(axis_at, parts):
        heights = jax.random.uniform(jax.random.fold_in(jax.random.fold_in(own_key, 6), axis_at), (parts,), jnp.float32, low / len(shards), top_value / len(shards))
        return jnp.repeat(jnp.exp(heights), extent[axis_at] // parts).reshape((-1,) + (1,) * (len(extent) - axis_at - 1))

    gain = one(*shards[0])
    for cut in shards[1:]:
        gain = gain * one(*cut)
    return gain


def normal_values(own_key, shape, spread, reach, cuts=(), kind=jnp.bfloat16):
    loudness = levels(own_key, shape, cuts, -0.22, 0.18) if cuts else 1.0
    result = jax.random.normal(own_key, shape, jnp.float32) * spread * loudness
    return jnp.minimum(jnp.maximum(result, -reach), reach).astype(kind)


def setup_inputs(seed: int = 0) -> dict:
    key_list = jax.random.split(jax.random.key(seed), 12)
    return {
        "model_state": normal_values(key_list[0], (MEMBERS, L, F, NLAT, NLON), 1.0, 6.0, ((0, 4), (1, 8)), jnp.float32),
        "noise_field": normal_values(key_list[1], (MEMBERS, L, F, NLAT, NLON), 1.0, 5.0, ((0, 4), (1, 8))),
        "cotangent": normal_values(key_list[2], (MEMBERS, L, F, NLAT, NLON), 1.0, 6.0, ((0, 4), (1, 8))),
        "zonal_shift": jnp.clip(jax.random.uniform(key_list[3], (L, F), jnp.float32, -0.02, 0.02) * levels(key_list[3], (L, F), ((0, 8),), -0.4, 0.0), -0.02, 0.02),
        "viscosity": jnp.clip(jnp.exp(math.log(3.0) - 3.4011974 * jax.random.uniform(key_list[4], (L, F), jnp.float32) ** levels(key_list[4], (L, F), ((0, 8),), -0.2, 0.2)), 0.1, 3.0),
        "noise_scale": jnp.clip(0.2 + 0.8 * jax.random.uniform(key_list[5], (L, F), jnp.float32) ** levels(key_list[5], (L, F), ((0, 8),), -0.2, 0.2), 0.2, 1.0),
        "w_in": normal_values(key_list[6], (HIN, H), HIN ** -0.5, 0.5),
        "b_in": normal_values(key_list[7], (H,), 0.5, 3.0, (), jnp.float32),
        "w_mid": normal_values(key_list[8], (H, H), H ** -0.5, 0.3125),
        "b_mid": normal_values(key_list[9], (H,), 0.5, 3.0, (), jnp.float32),
        "w_out": normal_values(key_list[10], (H, HOUT), H ** -0.5, 0.3125),
    }


def spectral_tables(lat_count, lon_count):
    lon_index = jnp.arange(lon_count, dtype=jnp.float32)
    wave_index = jnp.arange(WAVES, dtype=jnp.float32)
    phases = 2.0 * jnp.pi * lon_index[:, None] * wave_index[None, :] / lon_count
    lon_fwd = jnp.concatenate([jnp.cos(phases), jnp.sin(phases)], axis=1)
    wave_weight = jnp.where(wave_index == 0, 1.0, 2.0) / lon_count
    lon_inv = lon_fwd * jnp.concatenate([wave_weight, wave_weight])[None, :]
    lat_index = jnp.arange(lat_count, dtype=jnp.float32)
    mode_index = jnp.arange(MODES, dtype=jnp.float32)
    lat_fwd = jnp.cos(jnp.pi * (lat_index[:, None] + 0.5) * mode_index[None, :] / lat_count)
    lat_inv = lat_fwd * (jnp.where(mode_index == 0, 1.0, 2.0) / lat_count)[None, :]
    return (lon_fwd, lon_inv, lat_fwd, lat_inv)

def spectral_step(fields, zonal_shift, viscosity):
    lon_fwd, lon_inv, lat_fwd, lat_inv = spectral_tables(fields.shape[3], fields.shape[4])
    highest = lax.Precision.HIGHEST
    partial_lon = jnp.einsum('mlfij,jk->mlfik', fields, lon_fwd, precision=highest)
    spectrum = jnp.einsum('mlfik,ip->mlfpk', partial_lon, lat_fwd, precision=highest)
    wave_index = jnp.arange(WAVES, dtype=jnp.float32)
    mode_index = jnp.arange(MODES, dtype=jnp.float32)
    radial = (wave_index / WAVES)[None, :] ** 2 + (mode_index / MODES)[:, None] ** 2
    damping = jnp.exp(-viscosity[:, :, None, None] * radial[None, None])
    phases = zonal_shift[:, :, None, None] * wave_index[None, None, None, :]
    cosine = jnp.cos(phases) * damping
    sine = jnp.sin(phases) * damping
    cos_part = spectrum[..., :WAVES]
    sin_part = spectrum[..., WAVES:]
    rotated = jnp.concatenate([cos_part * cosine - sin_part * sine, cos_part * sine + sin_part * cosine], axis=-1)
    halfway = jnp.einsum('mlfpk,ip->mlfik', rotated, lat_inv, precision=highest)
    return jnp.einsum('mlfik,jk->mlfij', halfway, lon_inv, precision=highest)

def silu_slope(values):
    sigmoid = jax.nn.sigmoid(values)
    return sigmoid * (1.0 + values * (1.0 - sigmoid))

def reference(model_state, noise_field, cotangent, zonal_shift, viscosity, noise_scale, w_in, b_in, w_mid, b_mid, w_out):
    hidden = w_in.shape[1]
    inputs_count = w_in.shape[0]
    norm_scale = 1.0 / math.sqrt(MEMBERS * NLAT * NLON)

    def member_step(carry, members_in):
        state_one, noise_one, cotan_one = members_in
        dynamics = spectral_step(state_one[None], zonal_shift, viscosity)[0]
        level_shape = dynamics.shape
        inputs_bf = dynamics.astype(jnp.bfloat16).reshape(inputs_count, -1)
        pre_one = jnp.dot(w_in.T, inputs_bf, preferred_element_type=jnp.float32) + b_in[:, None]
        act_one = jax.nn.silu(pre_one).astype(jnp.bfloat16)
        pre_two = jnp.dot(w_mid.T, act_one, preferred_element_type=jnp.float32) + b_mid[:, None]
        act_two = jax.nn.silu(pre_two).astype(jnp.bfloat16)
        tendency = jnp.dot(w_out.T, act_two, preferred_element_type=jnp.float32).astype(jnp.bfloat16)
        factor = 1.0 + noise_scale[:, :, None, None] * noise_one.astype(jnp.float32)
        next_one = dynamics + tendency.astype(jnp.float32).reshape(level_shape) * factor
        grad_tend = (cotan_one.astype(jnp.float32) * factor).astype(jnp.bfloat16).reshape(inputs_count, -1)
        gw_out = jnp.dot(grad_tend, act_two.T, preferred_element_type=jnp.float32)
        slope_two = (jnp.dot(w_out, grad_tend, preferred_element_type=jnp.float32) * silu_slope(pre_two)).astype(jnp.bfloat16)
        gw_mid = jnp.dot(act_one, slope_two.T, preferred_element_type=jnp.float32)
        slope_one = (jnp.dot(w_mid, slope_two, preferred_element_type=jnp.float32) * silu_slope(pre_one)).astype(jnp.bfloat16)
        gw_in = jnp.dot(inputs_bf, slope_one.T, preferred_element_type=jnp.float32)
        gbias = jnp.stack([lax.optimization_barrier(jnp.sum(slope_one.astype(jnp.float32), axis=1)), lax.optimization_barrier(jnp.sum(slope_two.astype(jnp.float32), axis=1))])
        back_inputs = jnp.dot(w_in, slope_one, preferred_element_type=jnp.float32).astype(jnp.bfloat16)
        grad_levels = cotan_one.astype(jnp.float32) + back_inputs.astype(jnp.float32).reshape(level_shape)
        unused, pullback = jax.vjp(lambda fields: spectral_step(fields, zonal_shift, viscosity), state_one[None])
        grad_one = pullback(grad_levels[None])[0][0]
        carry = (carry[0] + gw_in, carry[1] + gw_mid, carry[2] + gw_out, carry[3] + gbias)
        return (carry, (next_one, grad_one))
    start = (jnp.zeros((inputs_count, hidden), jnp.float32), jnp.zeros((hidden, hidden), jnp.float32), jnp.zeros((w_out.shape[1], hidden), jnp.float32), jnp.zeros((2, hidden), jnp.float32))
    sums, outputs = lax.scan(member_step, start, (model_state, noise_field, cotangent))
    next_state, state_grad = outputs
    return (next_state, state_grad, sums[0] * norm_scale, sums[1] * norm_scale, sums[2] * norm_scale, sums[3] * norm_scale)
```

```python
import math

import jax
import jax.numpy as jnp
import numpy as np
from jax import lax
from jax.experimental import pallas as pl
from jax.experimental.pallas import tpu as pltpu
from jax.sharding import PartitionSpec as P


WAVES = 128
MODES = 128
BF = jnp.bfloat16
F32 = jnp.float32


def dot(a, b):
    return lax.dot_general(a, b, (((1,), (0,)), ((), ())), preferred_element_type=F32)


def dot_t(a, b):
    return lax.dot_general(a, b, (((1,), (1,)), ((), ())), preferred_element_type=F32)


def split(x):
    hi = x.astype(BF)
    return hi, (x - hi.astype(F32)).astype(BF)


def dot3(a, b):
    return dot(a[0], b[0]) + (dot(a[1], b[0]) + dot(a[0], b[1]))


def host_split(table):
    table = table.astype(np.float32)
    hi = table.astype(BF)
    lo = (table - hi.astype(np.float32)).astype(BF)
    return np.ascontiguousarray(hi), np.ascontiguousarray(lo)


def spectral_tables(lat_count, lon_count):
    turn = (np.arange(lon_count)[:, None] * np.arange(WAVES)[None, :]) % lon_count
    angle = 2.0 * np.pi * turn / lon_count
    lon = np.concatenate([np.cos(angle), np.sin(angle)], axis=1)
    lat = np.cos(np.pi * (np.arange(lat_count)[:, None] + 0.5) * np.arange(MODES)[None, :] / lat_count)
    return lon, lat


def rotation_rows(zonal_shift, viscosity, lat_count, lon_count):
    shift = zonal_shift.reshape(-1, 1, 1)
    visc = viscosity.reshape(-1, 1, 1)
    wave = jnp.arange(WAVES, dtype=F32)
    mode = jnp.arange(MODES, dtype=F32)
    wave_scale = jnp.where(wave == 0, 1.0, 2.0) / lon_count
    mode_scale = jnp.where(mode == 0, 1.0, 2.0) / lat_count
    damp_k = (jnp.exp(-visc * ((wave / WAVES) ** 2)[None, None, :]) * wave_scale)
    cosine = jnp.cos(shift * wave[None, None, :]) * damp_k
    sine = jnp.sin(shift * wave[None, None, :]) * damp_k
    damp_p = jnp.exp(-visc * ((mode / MODES) ** 2)[None, :, None]) * mode_scale[None, :, None]
    return cosine, sine, damp_p


def rotate(spec, cos_ref, sin_ref, damp_ref, sign):
    cosine = cos_ref[0]
    sine = sin_ref[0] * sign
    a = spec[:, :WAVES] * damp_ref[0]
    b = spec[:, WAVES:] * damp_ref[0]
    return jnp.concatenate([a * cosine - b * sine, a * sine + b * cosine], axis=1)


def pair(h_ref, l_ref):
    return h_ref[...], l_ref[...]


def spectral_fwd_kernel(x_ref, c_ref, s_ref, d_ref, fh, fl, fth, ftl, ah, al, ath, atl, half_ref, dyn_ref):
    z = dot3(split(x_ref[0]), pair(fh, fl))
    spec = dot3(pair(ath, atl), split(z))
    rot = rotate(spec, c_ref, s_ref, d_ref, 1.0)
    half = split(dot3(pair(ah, al), split(rot)))
    half_ref[0] = half[0]
    dyn_ref[0] = dot3(half, pair(fth, ftl))


def cot_spec_kernel(x_ref, fh, fl, ath, atl, out_ref):
    x = x_ref[0]
    z = dot(x, fh[...]) + dot(x, fl[...])
    out_ref[0] = dot3(pair(ath, atl), split(z))


def spectral_bwd_kernel(b_ref, g_ref, c_ref, s_ref, d_ref, fth, ftl, ah, al, ath, atl, out_ref):
    b = b_ref[0]
    spec = dot(ath[...], b) + dot(atl[...], b) + g_ref[0]
    rot = rotate(spec, c_ref, s_ref, d_ref, -1.0)
    half = split(dot3(pair(ah, al), split(rot)))
    out_ref[0] = dot3(half, pair(fth, ftl))


def grad_tend_kernel(noise_ref, cot_ref, ns_ref, out_ref):
    factor = 1.0 + ns_ref[...] * noise_ref[...].astype(F32)
    out_ref[0] = jnp.swapaxes(cot_ref[...].astype(F32) * factor, 0, 1).astype(BF)


def next_state_kernel(tend_ref, dyn_ref, noise_ref, ns_ref, *rest):
    out_ref = rest[-1]
    factor = 1.0 + ns_ref[...] * noise_ref[...].astype(F32)
    tend = jnp.swapaxes(tend_ref[0].astype(F32), 0, 1)
    out_ref[...] = dyn_ref[...] + tend * factor


def sigmoid(x):
    return 0.5 * jnp.tanh(0.5 * x) + 0.5


def gather_rows(ref, rows):
    parts = []
    for row in range(rows):
        v = ref[:, row]
        parts.append(v.reshape(v.shape[0] * v.shape[1], v.shape[2]))
    return parts


def inputs_of(half_ref, fth, ftl, rows):
    parts = []
    for h in gather_rows(half_ref, rows):
        parts.append((dot(h, fth[...]) + dot(h, ftl[...])).astype(BF))
    return jnp.concatenate(parts, axis=1)


def columns_fwd_kernel(half_ref, fth, ftl, w_in_t, b_in, w_mid_t, b_mid, w_out_t, out_ref):
    groups, rows, per_group, lon_count = out_ref.shape
    inputs = inputs_of(half_ref, fth, ftl, rows)
    pre_one = dot(w_in_t[...], inputs) + b_in[...]
    act_one = (pre_one * sigmoid(pre_one)).astype(BF)
    pre_two = dot(w_mid_t[...], act_one) + b_mid[...]
    act_two = (pre_two * sigmoid(pre_two)).astype(BF)
    tend = dot(w_out_t[...], act_two).astype(BF)
    for row in range(rows):
        part = tend[:, row * lon_count : (row + 1) * lon_count]
        out_ref[:, row] = part.reshape(groups, per_group, lon_count)


def lane_sums(x):
    total = x[:, :128]
    for at in range(128, x.shape[1], 128):
        total = total + x[:, at : at + 128]
    return total


def columns_bwd_kernel(
    half_ref, grad_ref, acc_in, bias_in, fth, ftl, fh, w_in_t, b_in, w_mid_t, b_mid, w_in, w_mid, w_out, *rest
):
    back_ref, acc_ref, bias_ref = rest[-3:]
    groups, rows, per_group, lon_count = grad_ref.shape
    ein = w_in.shape[0]
    hid = w_mid.shape[0]

    @pl.when(pl.program_id(0) == 0)
    def _():
        acc_ref[...] = acc_in[...]
        bias_ref[...] = bias_in[...]

    inputs = inputs_of(half_ref, fth, ftl, rows)
    grad = jnp.concatenate(gather_rows(grad_ref, rows), axis=1)
    pre_one = dot(w_in_t[...], inputs) + b_in[...]
    sig_one = sigmoid(pre_one)
    full_one = pre_one * sig_one
    act_one = full_one.astype(BF)
    silu_one = sig_one + full_one * (1.0 - sig_one)
    pre_two = dot(w_mid_t[...], act_one) + b_mid[...]
    sig_two = sigmoid(pre_two)
    full_two = pre_two * sig_two
    act_two = full_two.astype(BF)
    slope_two_f = dot(w_out[...], grad) * (sig_two + full_two * (1.0 - sig_two))
    slope_two = slope_two_f.astype(BF)
    slope_one_f = dot(w_mid[...], slope_two) * silu_one
    slope_one = slope_one_f.astype(BF)
    bias_ref[:, :128] += lane_sums(slope_one_f)
    bias_ref[:, 128:] += lane_sums(slope_two_f)
    acc_ref[:, :ein] += dot_t(slope_one, inputs)
    acc_ref[:, ein : ein + hid] += dot_t(slope_two, act_one)
    acc_ref[:, ein + hid :] += dot_t(act_two, grad)
    back = dot(w_in[...], slope_one).astype(BF)
    for row in range(rows):
        part = back[:, row * lon_count : (row + 1) * lon_count]
        out = dot(part, fh[...]).astype(BF)
        back_ref[:, row] = out.reshape(groups, per_group, out.shape[1])


def whole_spec(shape):
    return pl.BlockSpec(shape, lambda *_: (0,) * len(shape))


def call(kernel, grid, in_specs, out_specs, out_shape, flops, args, aliases=None):
    return pl.pallas_call(
        kernel,
        grid=grid,
        in_specs=in_specs,
        out_specs=out_specs,
        out_shape=out_shape,
        input_output_aliases=aliases or {},
        cost_estimate=pl.CostEstimate(flops=flops, transcendentals=0, bytes_accessed=1 << 22),
        compiler_params=pltpu.CompilerParams(
            dimension_semantics=("arbitrary",) * len(grid), vmem_limit_bytes=56 << 20
        ),
    )(*args)


def per_device(
    model_state, noise_field, cotangent, zonal_shift, viscosity, noise_scale, w_in, b_in, w_mid, b_mid, w_out
):
    members_here, levels, fields, nlat, nlon = model_state.shape
    groups = lax.axis_size("level")
    members = lax.axis_size("member")
    lf = levels * fields
    own = nlat // groups
    part = own // 2
    ein, hid = w_in.shape
    state = model_state.reshape(lf, nlat, nlon)
    noise = noise_field.reshape(lf, nlat, nlon)
    cot = cotangent.reshape(lf, nlat, nlon)
    scale = noise_scale.reshape(lf, 1, 1)
    lon, lat = spectral_tables(nlat, nlon)
    fh, fl = host_split(lon)
    fth, ftl = host_split(lon.T)
    ah, al = host_split(lat)
    ath, atl = host_split(lat.T)
    waves2 = fh.shape[1]

    def sds(shape, dtype):
        return jax.ShapeDtypeStruct(shape, dtype)

    def grad_part(which):
        at = pl.BlockSpec((lf, part, nlon), lambda s: (0, 2 * s + which, 0))
        return call(
            grad_tend_kernel,
            (groups,),
            [at, at, whole_spec((lf, 1, 1))],
            pl.BlockSpec((1, part, lf, nlon), lambda s: (s, 0, 0, 0)),
            sds((groups, part, lf, nlon), BF),
            10**9,
            (noise, cot, scale),
        )

    def exchange(x, axis="level"):
        return lax.all_to_all(x, axis, split_axis=0, concat_axis=0, tiled=True)

    per_lf = lambda *shape: pl.BlockSpec((1,) + shape, lambda s: (s,) + (0,) * len(shape))
    row_spec = per_lf(1, WAVES)
    col_spec = per_lf(MODES, 1)
    f_specs = [whole_spec(fh.shape)] * 2
    ft_specs = [whole_spec(fth.shape)] * 2
    a_specs = [whole_spec(ah.shape)] * 2
    at_specs = [whole_spec(ath.shape)] * 2

    def ordered(value, *after):
        return lax.optimization_barrier((value,) + after)[0]

    grad_one_send = grad_part(0)
    grad_one = exchange(grad_one_send)
    state, shift, visc, _ = lax.optimization_barrier((state, zonal_shift, viscosity, grad_one_send))
    cosine, sine, damp_p = rotation_rows(shift, visc, nlat, nlon)
    half, dyn = call(
        spectral_fwd_kernel,
        (lf,),
        [per_lf(nlat, nlon), row_spec, row_spec, col_spec] + f_specs + ft_specs + a_specs + at_specs,
        [per_lf(nlat, waves2), per_lf(nlat, nlon)],
        [sds((lf, nlat, waves2), BF), sds((lf, nlat, nlon), F32)],
        2 * 10**10,
        (state, cosine, sine, damp_p, fh, fl, fth, ftl, ah, al, ath, atl),
    )
    send = half.reshape(lf, groups, own, waves2).transpose(1, 2, 0, 3)
    cols = exchange(ordered(send, grad_one))
    grad_two_send = grad_part(1)
    grad_two = exchange(ordered(grad_two_send, cols))
    cot_spec = call(
        cot_spec_kernel,
        (lf,),
        [per_lf(nlat, nlon)] + f_specs + at_specs,
        per_lf(MODES, waves2),
        sds((lf, MODES, waves2), F32),
        10**10,
        (cot, fh, fl, ath, atl),
    )

    w_in_t = w_in.T
    w_mid_t = w_mid.T
    w_out_t = w_out.T
    bias_one = b_in.reshape(hid, 1)
    bias_two = b_mid.reshape(hid, 1)
    step = 2
    steps = part // step

    def half_spec(which):
        return pl.BlockSpec((groups, step, lf, waves2), lambda s: (0, s + which * steps, 0, 0))

    grid_spec = pl.BlockSpec((groups, step, lf, nlon), lambda s: (0, s, 0, 0))

    def forward(which):
        return call(
            columns_fwd_kernel,
            (steps,),
            [half_spec(which)]
            + ft_specs
            + [whole_spec(v.shape) for v in (w_in_t, bias_one, w_mid_t, bias_two, w_out_t)],
            grid_spec,
            sds((groups, part, lf, nlon), BF),
            10**10,
            (cols, fth, ftl, w_in_t, bias_one, w_mid_t, bias_two, w_out_t),
        )

    acc_shape = (hid, 2 * ein + hid)
    sums_shape = (hid, 256)

    def backward(which, grads, acc, sums, before):
        specs = (
            [half_spec(which), grid_spec, whole_spec(acc_shape), whole_spec(sums_shape)]
            + ft_specs
            + [whole_spec(fh.shape)]
            + [whole_spec(v.shape) for v in (w_in_t, bias_one, w_mid_t, bias_two, w_in, w_mid, w_out)]
        )
        args = (cols, grads, acc, sums, fth, ftl, fh, w_in_t, bias_one, w_mid_t, bias_two, w_in, w_mid, w_out)
        aliases = {}
        if before is not None:
            aliases = {len(args): 0}
            specs = specs + [pl.BlockSpec(memory_space=pl.ANY)]
            args = args + (before,)
        return call(
            columns_bwd_kernel,
            (steps,),
            specs,
            [half_spec(which), whole_spec(acc_shape), whole_spec(sums_shape)],
            [sds((groups, own, lf, waves2), BF), sds(acc_shape, F32), sds(sums_shape, F32)],
            3 * 10**10,
            args,
            aliases,
        )

    tend_one_send = forward(0)
    tend_one = exchange(ordered(tend_one_send, grad_two))
    back, acc, sums = backward(0, grad_one, jnp.zeros(acc_shape, F32), jnp.zeros(sums_shape, F32), None)
    tend_two_send = forward(1)
    back, acc, sums = backward(1, grad_two, acc, sums, back)
    back = exchange(ordered(back, tend_one))

    def reduce_axis(x, axis):
        size = lax.axis_size(axis)
        at = lax.axis_index(axis)
        total = lax.dynamic_index_in_dim(x, at, 0, keepdims=False)
        for hop in range(1, size):
            block = lax.dynamic_index_in_dim(x, (at + hop) % size, 0, keepdims=False)
            total = total + lax.ppermute(block, axis, [(s, (s + hop) % size) for s in range(size)])
        return total

    sums_two = jnp.stack([jnp.sum(sums[:, :128], axis=1), jnp.sum(sums[:, 128:], axis=1)], axis=1)
    packed = jnp.concatenate([acc, sums_two], axis=1)
    width = packed.shape[1]
    share = hid // (groups * members)
    packed = packed.reshape(groups, members, share, width).transpose(1, 0, 2, 3)
    packed = reduce_axis(packed, "member")
    packed = reduce_axis(packed, "level")
    packed = packed * (1.0 / math.sqrt(members_here * members * nlat * nlon))
    packed = packed.T
    tend_two = exchange(ordered(tend_two_send, back, packed))

    def finish(which, tend, before):
        rows = pl.BlockSpec((lf, part, nlon), lambda s: (0, 2 * s + which, 0))
        specs = [pl.BlockSpec((1, part, lf, nlon), lambda s: (s, 0, 0, 0)), rows, rows, whole_spec((lf, 1, 1))]
        args = (tend, dyn, noise, scale)
        aliases = {}
        if before is not None:
            aliases = {len(args): 0}
            specs = specs + [pl.BlockSpec(memory_space=pl.ANY)]
            args = args + (before,)
        return call(
            next_state_kernel, (groups,), specs, rows, sds((lf, nlat, nlon), F32), 10**10, args, aliases
        )

    next_state = finish(0, tend_one, None)
    state_grad = call(
        spectral_bwd_kernel,
        (lf,),
        [per_lf(nlat, waves2), per_lf(MODES, waves2), row_spec, row_spec, col_spec]
        + ft_specs
        + a_specs
        + at_specs,
        per_lf(nlat, nlon),
        sds((lf, nlat, nlon), F32),
        2 * 10**10,
        (
            back.reshape(nlat, lf, waves2).transpose(1, 0, 2),
            cot_spec, cosine, sine, damp_p, fth, ftl, ah, al, ath, atl,
        ),
    )
    next_state = finish(1, tend_two, next_state)

    shape = model_state.shape
    return (
        next_state.reshape(shape),
        state_grad.reshape(shape),
        packed[:ein],
        packed[ein : ein + hid],
        packed[ein + hid : 2 * ein + hid],
        packed[2 * ein + hid :],
    )


def solution(mesh):
    big = P("member", "level", None, None, None)
    small = P("level", None)
    grads = P(None, ("level", "member"))
    return jax.shard_map(
        per_device,
        mesh=mesh,
        in_specs=(big, big, big, small, small, small, P(), P(), P(), P(), P()),
        out_specs=(big, big, grads, grads, grads, grads),
        check_vma=False,
    )
```

```python
import math

import jax
import jax.numpy as jnp
import numpy as np
from jax import lax
from jax.experimental import pallas as pl
from jax.experimental.pallas import tpu as pltpu
from jax.sharding import PartitionSpec as P


WAVES = 128
MODES = 128
BF = jnp.bfloat16
F32 = jnp.float32


def dot(a, b):
    return lax.dot_general(a, b, (((1,), (0,)), ((), ())), preferred_element_type=F32)


def dot_t(a, b):
    return lax.dot_general(a, b, (((1,), (1,)), ((), ())), preferred_element_type=F32)


def split(x):
    hi = x.astype(BF)
    return hi, (x - hi.astype(F32)).astype(BF)


def dot3(a, b):
    return dot(a[0], b[0]) + (dot(a[1], b[0]) + dot(a[0], b[1]))


def host_split(table):
    table = table.astype(np.float32)
    hi = table.astype(BF)
    lo = (table - hi.astype(np.float32)).astype(BF)
    return np.ascontiguousarray(hi), np.ascontiguousarray(lo)


def spectral_tables(lat_count, lon_count):
    turn = (np.arange(lon_count)[:, None] * np.arange(WAVES)[None, :]) % lon_count
    angle = 2.0 * np.pi * turn / lon_count
    lon = np.concatenate([np.cos(angle), np.sin(angle)], axis=1)
    lat = np.cos(np.pi * (np.arange(lat_count)[:, None] + 0.5) * np.arange(MODES)[None, :] / lat_count)
    return lon, lat


def rotation_rows(zonal_shift, viscosity, lat_count, lon_count):
    shift = zonal_shift.reshape(-1, 1, 1)
    visc = viscosity.reshape(-1, 1, 1)
    wave = jnp.arange(WAVES, dtype=F32)
    mode = jnp.arange(MODES, dtype=F32)
    wave_scale = jnp.where(wave == 0, 1.0, 2.0) / lon_count
    mode_scale = jnp.where(mode == 0, 1.0, 2.0) / lat_count
    damp_k = (jnp.exp(-visc * ((wave / WAVES) ** 2)[None, None, :]) * wave_scale)
    cosine = jnp.cos(shift * wave[None, None, :]) * damp_k
    sine = jnp.sin(shift * wave[None, None, :]) * damp_k
    damp_p = jnp.exp(-visc * ((mode / MODES) ** 2)[None, :, None]) * mode_scale[None, :, None]
    return cosine, sine, damp_p


def rotate(spec, cos_ref, sin_ref, damp_ref, sign):
    cosine = cos_ref[0]
    sine = sin_ref[0] * sign
    a = spec[:, :WAVES] * damp_ref[0]
    b = spec[:, WAVES:] * damp_ref[0]
    return jnp.concatenate([a * cosine - b * sine, a * sine + b * cosine], axis=1)


def pair(h_ref, l_ref):
    return h_ref[...], l_ref[...]


def swap_rows(x):
    return jnp.swapaxes(x.astype(F32), 0, 1)


def spectral_fwd_kernel(
    at_ref, x_ref, c_ref, s_ref, d_ref, fh, fl, fth, ftl, ah, al, ath, atl, dyn_ref, *rest
):
    outs, keep = rest[:-1], rest[-1]
    groups = len(outs)
    own = keep.shape[2]
    z = dot3(split(x_ref[0]), pair(fh, fl))
    spec = dot3(pair(ath, atl), split(z))
    rot = rotate(spec, c_ref, s_ref, d_ref, 1.0)
    half = split(dot3(pair(ah, al), split(rot)))
    dyn_ref[0] = dot3(half, pair(fth, ftl))
    step = pl.program_id(0)
    for g in range(groups):
        keep[step, g] = half[0][g * own : (g + 1) * own]

    @pl.when(step == pl.num_programs(0) - 1)
    def _():
        for hop in range(groups):
            dest = lax.rem(at_ref[0] + hop, groups)
            outs[hop][...] = swap_rows(keep[:, dest]).astype(BF)


def cot_spec_kernel(x_ref, fh, fl, ath, atl, out_ref):
    x = x_ref[0]
    z = dot(x, fh[...]) + dot(x, fl[...])
    out_ref[0] = dot3(pair(ath, atl), split(z))


def spectral_bwd_kernel(g_ref, c_ref, s_ref, d_ref, fth, ftl, ah, al, ath, atl, *rest):
    backs, out_ref, keep = rest[:-2], rest[-2], rest[-1]
    own = backs[0].shape[0]
    step = pl.program_id(0)

    @pl.when(step == 0)
    def _():
        for hop, ref in enumerate(backs):
            keep[:, hop * own : (hop + 1) * own, :] = swap_rows(ref[...]).astype(BF)

    b = keep[step]
    spec = dot(ath[...], b) + dot(atl[...], b) + g_ref[0]
    rot = rotate(spec, c_ref, s_ref, d_ref, -1.0)
    half = split(dot3(pair(ah, al), split(rot)))
    out_ref[0] = dot3(half, pair(fth, ftl))


def grad_tend_kernel(at_ref, noise_ref, cot_ref, ns_ref, *outs):
    groups = len(outs)
    for hop in range(groups):
        dest = lax.rem(at_ref[0] + hop, groups)
        factor = 1.0 + ns_ref[...] * noise_ref[:, dest].astype(F32)
        outs[hop][...] = swap_rows(cot_ref[:, dest].astype(F32) * factor).astype(BF)


def next_state_kernel(at_ref, dyn_ref, noise_ref, ns_ref, *rest):
    groups = dyn_ref.shape[1]
    tends, out_ref = rest[:groups], rest[-1]
    for hop in range(groups):
        src = lax.rem(at_ref[0] + (groups - hop), groups)
        factor = 1.0 + ns_ref[...] * noise_ref[:, src].astype(F32)
        out_ref[:, src] = dyn_ref[:, src] + swap_rows(tends[hop][...]) * factor


def sigmoid(x):
    return 0.5 * jnp.tanh(0.5 * x) + 0.5


def rows_of(refs, row):
    return jnp.concatenate([ref[row] for ref in refs], axis=0)


def inputs_of(halves, fth, ftl, rows):
    parts = []
    for row in range(rows):
        h = rows_of(halves, row)
        parts.append((dot(h, fth[...]) + dot(h, ftl[...])).astype(BF))
    return jnp.concatenate(parts, axis=1)


def columns_fwd_kernel(fth, ftl, w_in_t, b_in, w_mid_t, b_mid, w_out_t, *rest):
    groups = len(rest) // 2
    halves, outs = rest[:groups], rest[groups:]
    rows, per_group, lon_count = outs[0].shape
    inputs = inputs_of(halves, fth, ftl, rows)
    pre_one = dot(w_in_t[...], inputs) + b_in[...]
    act_one = (pre_one * sigmoid(pre_one)).astype(BF)
    pre_two = dot(w_mid_t[...], act_one) + b_mid[...]
    act_two = (pre_two * sigmoid(pre_two)).astype(BF)
    tend = dot(w_out_t[...], act_two).astype(BF)
    for hop, ref in enumerate(outs):
        for row in range(rows):
            ref[row] = tend[hop * per_group : (hop + 1) * per_group, row * lon_count : (row + 1) * lon_count]


def lane_sums(x):
    total = x[:, :128]
    for at in range(128, x.shape[1], 128):
        total = total + x[:, at : at + 128]
    return total


def columns_bwd_kernel(
    acc_in, bias_in, fth, ftl, fh, w_in_t, b_in, w_mid_t, b_mid, w_in, w_mid, w_out, groups, *rest
):
    halves, grads = rest[:groups], rest[groups : 2 * groups]
    backs = rest[-groups - 2 : -2]
    acc_ref, bias_ref = rest[-2:]
    rows, per_group, lon_count = grads[0].shape
    ein = w_in.shape[0]
    hid = w_mid.shape[0]

    @pl.when(pl.program_id(0) == 0)
    def _():
        acc_ref[...] = acc_in[...]
        bias_ref[...] = bias_in[...]

    inputs = inputs_of(halves, fth, ftl, rows)
    grad = jnp.concatenate([rows_of(grads, row) for row in range(rows)], axis=1)
    pre_one = dot(w_in_t[...], inputs) + b_in[...]
    sig_one = sigmoid(pre_one)
    full_one = pre_one * sig_one
    act_one = full_one.astype(BF)
    silu_one = sig_one + full_one * (1.0 - sig_one)
    pre_two = dot(w_mid_t[...], act_one) + b_mid[...]
    sig_two = sigmoid(pre_two)
    full_two = pre_two * sig_two
    act_two = full_two.astype(BF)
    slope_two_f = dot(w_out[...], grad) * (sig_two + full_two * (1.0 - sig_two))
    slope_two = slope_two_f.astype(BF)
    slope_one_f = dot(w_mid[...], slope_two) * silu_one
    slope_one = slope_one_f.astype(BF)
    bias_ref[:, :128] += lane_sums(slope_one_f)
    bias_ref[:, 128:] += lane_sums(slope_two_f)
    acc_ref[:, :ein] += dot_t(slope_one, inputs)
    acc_ref[:, ein : ein + hid] += dot_t(slope_two, act_one)
    acc_ref[:, ein + hid :] += dot_t(act_two, grad)
    back = dot(w_in[...], slope_one).astype(BF)
    for row in range(rows):
        part = back[:, row * lon_count : (row + 1) * lon_count]
        out = dot(part, fh[...]).astype(BF)
        for hop, ref in enumerate(backs):
            ref[row] = out[hop * per_group : (hop + 1) * per_group]


def whole_spec(shape):
    return pl.BlockSpec(shape, lambda *_: (0,) * len(shape))


def call(kernel, grid, in_specs, out_specs, out_shape, flops, args, aliases=None, prefetch=0, scratch=()):
    return pl.pallas_call(
        kernel,
        grid_spec=pltpu.PrefetchScalarGridSpec(
            num_scalar_prefetch=prefetch,
            grid=grid,
            in_specs=in_specs,
            out_specs=out_specs,
            scratch_shapes=list(scratch),
        ),
        out_shape=out_shape,
        input_output_aliases=aliases or {},
        cost_estimate=pl.CostEstimate(flops=flops, transcendentals=0, bytes_accessed=1 << 22),
        compiler_params=pltpu.CompilerParams(
            dimension_semantics=("arbitrary",) * len(grid), vmem_limit_bytes=56 << 20
        ),
    )(*args)


def per_device(
    model_state, noise_field, cotangent, zonal_shift, viscosity, noise_scale, w_in, b_in, w_mid, b_mid, w_out
):
    members_here, levels, fields, nlat, nlon = model_state.shape
    groups = lax.axis_size("level")
    members = lax.axis_size("member")
    lf = levels * fields
    own = nlat // groups
    part = own // 2
    ein, hid = w_in.shape
    state = model_state.reshape(lf, nlat, nlon)
    noise = noise_field.reshape(lf, nlat, nlon)
    cot = cotangent.reshape(lf, nlat, nlon)
    scale = noise_scale.reshape(lf, 1, 1)
    lon, lat = spectral_tables(nlat, nlon)
    fh, fl = host_split(lon)
    ah, al = host_split(lat)
    ath, atl = host_split(lat.T)
    waves2 = fh.shape[1]

    def sds(shape, dtype):
        return jax.ShapeDtypeStruct(shape, dtype)

    at = lax.axis_index("level").astype(jnp.int32)
    at_one = at.reshape(1)
    chunk = 8

    def send_order(x):
        blocks = x.reshape((groups, -1) + x.shape[1:])
        blocks = jnp.concatenate([blocks, blocks], axis=0)
        return lax.dynamic_slice_in_dim(blocks, at, groups, 0).reshape(x.shape)

    def recv_order(x):
        blocks = x.reshape((groups, -1) + x.shape[1:])
        blocks = jnp.concatenate([blocks[:1], blocks[:0:-1]], axis=0)
        blocks = jnp.concatenate([blocks, blocks], axis=0)
        return lax.dynamic_slice_in_dim(blocks, (groups - at) % groups, groups, 0).reshape(x.shape)

    def rows_block(which):
        return pl.BlockSpec((lf, groups, chunk, nlon), lambda s, _: (0, 0, s + which * (part // chunk), 0))

    by_group = (lf, groups, own, nlon)

    def grad_part(which, *after):
        noise_here, cot_here = noise, cot
        if after:
            noise_here, cot_here = lax.optimization_barrier((noise, cot) + after)[:2]
        return call(
            grad_tend_kernel,
            (part // chunk,),
            [rows_block(which), rows_block(which), whole_spec((lf, 1, 1))],
            [pl.BlockSpec((chunk, lf, nlon), lambda s, _: (s, 0, 0))] * groups,
            [sds((part, lf, nlon), BF)] * groups,
            10**9,
            (at_one, noise_here.reshape(by_group), cot_here.reshape(by_group), scale),
            prefetch=1,
        )

    def exchange(blocks):
        got = [blocks[0]]
        for hop in range(1, groups):
            got.append(lax.ppermute(blocks[hop], "level", [(s, (s + hop) % groups) for s in range(groups)]))
        return got

    per_lf = lambda *shape: pl.BlockSpec((1,) + shape, lambda s, *_: (s,) + (0,) * len(shape))
    row_spec = per_lf(1, WAVES)
    col_spec = per_lf(MODES, 1)
    f_specs = [whole_spec(fh.shape)] * 2
    ft_specs = [whole_spec(fh.shape[::-1])] * 2
    a_specs = [whole_spec(ah.shape)] * 2
    at_specs = [whole_spec(ath.shape)] * 2

    sends = grad_part(0)
    grad_one = exchange(sends)
    state, shift, visc, w_in, w_mid, w_out, at, fh, fl, _ = lax.optimization_barrier(
        (state, zonal_shift, viscosity, w_in, w_mid, w_out, at, jnp.asarray(fh), jnp.asarray(fl), sends[0])
    )
    fth, ftl = fh.T, fl.T
    cosine, sine, damp_p = rotation_rows(shift, visc, nlat, nlon)
    dyn, *sends = call(
        spectral_fwd_kernel,
        (lf,),
        [per_lf(nlat, nlon), row_spec, row_spec, col_spec] + f_specs + ft_specs + a_specs + at_specs,
        [per_lf(nlat, nlon)] + [whole_spec((own, lf, waves2))] * groups,
        [sds((lf, nlat, nlon), F32)] + [sds((own, lf, waves2), BF)] * groups,
        2 * 10**10,
        (at_one, state, cosine, sine, damp_p, fh, fl, fth, ftl, ah, al, ath, atl),
        prefetch=1,
        scratch=[pltpu.VMEM((lf, groups, own, waves2), BF)],
    )
    cols = exchange(sends)
    sends = grad_part(1, sends[0])
    held = lax.optimization_barrier((*sends, *cols))
    cols = held[groups:]
    grad_two = exchange(held[:groups])
    cot_spec = call(
        cot_spec_kernel,
        (lf,),
        [per_lf(nlat, nlon)] + f_specs + at_specs,
        per_lf(MODES, waves2),
        sds((lf, MODES, waves2), F32),
        10**10,
        (cot, fh, fl, ath, atl),
    )

    w_in_t = recv_order(w_in).T
    w_in_send = send_order(w_in)
    w_mid_t = w_mid.T
    w_out_t = w_out.T
    w_out_recv = recv_order(w_out_t).T
    w_out_t = send_order(w_out_t)
    bias_one = b_in.reshape(hid, 1)
    bias_two = b_mid.reshape(hid, 1)
    step = 2
    steps = part // step

    def half_spec(which):
        return pl.BlockSpec((step, lf, waves2), lambda s: (s + which * steps, 0, 0))

    grid_spec = pl.BlockSpec((step, lf, nlon), lambda s: (s, 0, 0))

    def forward(which):
        return call(
            columns_fwd_kernel,
            (steps,),
            ft_specs
            + [whole_spec(v.shape) for v in (w_in_t, bias_one, w_mid_t, bias_two, w_out_t)]
            + [half_spec(which)] * groups,
            [grid_spec] * groups,
            [sds((part, lf, nlon), BF)] * groups,
            10**10,
            (fth, ftl, w_in_t, bias_one, w_mid_t, bias_two, w_out_t, *cols),
        )

    acc_shape = (hid, 2 * ein + hid)
    sums_shape = (hid, 256)

    def backward(which, grads, acc, sums, before):
        args = (acc, sums, fth, ftl, fh, w_in_t, bias_one, w_mid_t, bias_two, w_in_send, w_mid, w_out_recv)
        specs = [whole_spec(v.shape) for v in args]
        args = args + (*cols, *grads)
        specs = specs + [half_spec(which)] * groups + [grid_spec] * groups
        aliases = {}
        if before is not None:
            aliases = {len(args) + hop: hop for hop in range(groups)}
            specs = specs + [pl.BlockSpec(memory_space=pl.ANY)] * groups
            args = args + tuple(before)
        *back, acc, sums = call(
            lambda *refs: columns_bwd_kernel(*refs[:12], groups, *refs[12:]),
            (steps,),
            specs,
            [half_spec(which)] * groups + [whole_spec(acc_shape), whole_spec(sums_shape)],
            [sds((own, lf, waves2), BF)] * groups + [sds(acc_shape, F32), sds(sums_shape, F32)],
            3 * 10**10,
            args,
            aliases,
        )
        return back, acc, sums

    sends_one = forward(0)
    back, acc, sums = backward(0, grad_one, jnp.zeros(acc_shape, F32), jnp.zeros(sums_shape, F32), None)
    *sends_one, sums = lax.optimization_barrier((*sends_one, sums))
    tend_one = exchange(sends_one)
    back, acc, sums = backward(1, grad_two, acc, sums, back)
    back = exchange(back)
    acc, *cols = lax.optimization_barrier((acc, *cols))
    sends_two = forward(1)

    def reduce_axis(x, axis):
        size = lax.axis_size(axis)
        at = lax.axis_index(axis)
        total = lax.dynamic_index_in_dim(x, at, 0, keepdims=False)
        for hop in range(1, size):
            block = lax.dynamic_index_in_dim(x, (at + hop) % size, 0, keepdims=False)
            total = total + lax.ppermute(block, axis, [(s, (s + hop) % size) for s in range(size)])
        return total

    sums_two = jnp.stack([jnp.sum(sums[:, :128], axis=1), jnp.sum(sums[:, 128:], axis=1)], axis=1)
    index = jnp.arange(ein)
    source = (at + groups - index // lf) % groups * lf + index % lf
    place = (source[:, None] == index[None, :]).astype(F32)
    sorted_in = jnp.dot(acc[:, :ein], place, precision=lax.Precision.HIGHEST)
    sorted_out = jnp.dot(acc[:, ein + hid :], place, precision=lax.Precision.HIGHEST)
    packed = jnp.concatenate([sorted_in, acc[:, ein : ein + hid], sorted_out, sums_two], axis=1)
    width = packed.shape[1]
    share = hid // (groups * members)
    packed = packed.reshape(groups, members, share, width).transpose(1, 0, 2, 3)
    packed = reduce_axis(packed, "member")
    packed = reduce_axis(packed, "level")
    packed = packed * (1.0 / math.sqrt(members_here * members * nlat * nlon))
    packed = packed.T
    tend_two = exchange(sends_two)

    def finish(which, tend, before):
        rows = rows_block(which)
        specs = [rows, rows, whole_spec((lf, 1, 1))]
        specs = specs + [pl.BlockSpec((chunk, lf, nlon), lambda s, _: (s, 0, 0))] * groups
        args = (at_one, dyn.reshape(by_group), noise.reshape(by_group), scale, *tend)
        aliases = {}
        if before is not None:
            aliases = {len(args): 0}
            specs = specs + [pl.BlockSpec(memory_space=pl.ANY)]
            args = args + (before,)
        return call(
            next_state_kernel, (part // chunk,), specs, rows, sds(by_group, F32), 10**10, args, aliases, prefetch=1
        )

    next_state = finish(0, tend_one, None)
    lat_recv = recv_order(jnp.concatenate([jnp.asarray(ah), jnp.asarray(al)], axis=1)).T
    state_grad = call(
        spectral_bwd_kernel,
        (lf,),
        [per_lf(MODES, waves2), row_spec, row_spec, col_spec]
        + ft_specs
        + a_specs
        + at_specs
        + [whole_spec((own, lf, waves2))] * groups,
        per_lf(nlat, nlon),
        sds((lf, nlat, nlon), F32),
        2 * 10**10,
        (cot_spec, cosine, sine, damp_p, fth, ftl, ah, al, lat_recv[:MODES], lat_recv[MODES:], *back),
        scratch=[pltpu.VMEM((lf, nlat, waves2), BF)],
    )
    next_state = finish(1, tend_two, next_state)

    shape = model_state.shape
    return (
        next_state.reshape(shape),
        state_grad.reshape(shape),
        packed[:ein],
        packed[ein : ein + hid],
        packed[ein + hid : 2 * ein + hid],
        packed[2 * ein + hid :],
    )


def solution(mesh):
    big = P("member", "level", None, None, None)
    small = P("level", None)
    grads = P(None, ("level", "member"))
    return jax.shard_map(
        per_device,
        mesh=mesh,
        in_specs=(big, big, big, small, small, small, P(), P(), P(), P(), P()),
        out_specs=(big, big, grads, grads, grads, grads),
        check_vma=False,
    )
```
